32 devices in a mesh: groups: 2 (over x), gx: 16 (over z, y, core).
Axes of the slice: x: 2, y: 2, z: 4, core: 2. Of those that a mesh axis runs over, the one named last changes fastest.
Arguments:
- points: bfloat16 [32, 6, 1, 128, 512], P(('groups', 'gx')), parts along dimension 0, may hold values from -6 to 6
- order: int32 [32, 6, 1, 128], P(('groups', 'gx')), parts along dimension 0, may hold values from 0 to 127, each once within a row
- masks: int32 [32, 6, 1, 26], P(('groups', 'gx')), parts along dimension 0, may hold values 0 or 1
- counts: int32 [32, 6, 1], P('groups'), parts along dimension 0, may hold values from 1 to 128
- gain: float32 [512], replicated, may hold values from 0.5 to 1.5
- shift_bias: float32 [512], replicated, may hold values from -3 to 3
- w_qkv: bfloat16 [512, 1536], replicated, may hold values from -1.5 to 1.5
- w_out: bfloat16 [512, 512], replicated, may hold values from -0.25 to 0.25
Outputs:
- result: bfloat16 [32, 6, 1, 128, 512], P(('groups', 'gx')), parts along dimension 0
The draws below stay inside these ranges and needn't reach their ends.
There are 2 independent parts, one for each index of `groups`. The reference program is written for one: setup_inputs(seed, part) draws one part's arguments, and reference() takes and returns one part's arrays. A program takes and returns all parts, laid end to end along the dimension named above; an argument that names none is the same for every part. Nothing has to cross between parts.
All inputs are finite; a program needn't handle non-finite values. No bound on the sum of `masks` on one device may be relied on, other than what follows from the above.
Results may differ from the reference program's by a relative error of at most 0.012.
Values may be sent and summed in bfloat16 or wider, within the bound.
A program may use at most 128 MiB of HBM per device.

```python
import jax
import jax.numpy as jnp
from jax import lax

D = 512
HEADS = 8
P_SIZE = 128
BY = 6
BZ = 1
NBX = 16


def bias_normal(key):
    values = jax.random.normal(jax.random.fold_in(key, 1701), (D,), jnp.float32)
    return jnp.clip(values, -6.0, 6.0)


def draw_shift_bias(key, part):
    return 0.5 * bias_normal(key)


def draw_w_qkv(key, part):
    spread = D ** (-0.5)
    noise = jax.random.normal(jax.random.fold_in(key, 1702), (D, 3 * D), jnp.float32) * spread
    noise = jnp.clip(noise, -6.0 * spread, 6.0 * spread)
    return noise.astype(jnp.bfloat16)


def plant(drawn, stream_key, least, top_value):
    shape = drawn.shape
    index_at = [jax.random.randint(jax.random.fold_in(stream_key, axis), (), 0, shape[axis]) for axis in range(len(shape))]
    drawn = drawn.at[tuple(index_at)].set(least)
    longest = shape.index(max(shape))
    index_at[longest] = (index_at[longest] + 1) % shape[longest]
    return drawn.at[tuple(index_at)].set(top_value)


def steps_of(own_key, dims, pieces, low, top_value):
    level, own = 1.0, jax.random.fold_in(own_key, 6)
    for position, parts in pieces:
        heights = jnp.exp(jax.random.uniform(jax.random.fold_in(own, position), (parts,), jnp.float32, low / len(pieces), top_value / len(pieces)))
        level = level * jnp.repeat(heights, dims[position] // parts).reshape([-1 if axis == position else 1 for axis in range(len(dims))])
    return level


def centred(key, extent, deviation, bound, split=(), kind=jnp.bfloat16):
    level = steps_of(key, extent, split, -0.22, 0.18) if split else 1.0
    array = jax.random.normal(key, extent, jnp.float32) * deviation * level
    return jnp.minimum(jnp.maximum(array, -bound), bound).astype(kind)


def setup_inputs(seed: int = 0, part: int = 0) -> dict:
    keys = jax.random.split(jax.random.key(seed), 9)
    part_splits = jax.random.split(jax.random.fold_in(keys[8], part), 9)
    points = centred(part_splits[0], (NBX, BY, BZ, P_SIZE, D), 1.0, 6.0, ((0, 16),))
    order = jax.vmap(lambda own: jax.random.permutation(own, P_SIZE))(jax.random.split(part_splits[1], NBX * BY * BZ)).reshape((NBX, BY, BZ, P_SIZE)).astype(jnp.int32)
    masks = plant((jax.random.randint(part_splits[2], (NBX, BY, BZ, 26), 0, 2) < 1).astype(jnp.int32), jax.random.fold_in(part_splits[2], 1), 0, 1)
    counts = plant(jax.random.randint(part_splits[3], (NBX, BY, BZ), 1, P_SIZE + 1), jax.random.fold_in(part_splits[3], 1), 1, P_SIZE).astype(jnp.int32)
    gain = jnp.clip(1.0 + 0.1 * jax.random.normal(keys[4], (D,), jnp.float32), 0.5, 1.5)
    shift_bias = draw_shift_bias(jax.random.fold_in(keys[8], 71), part)
    w_qkv = draw_w_qkv(jax.random.fold_in(keys[8], 71), part)
    w_out = centred(keys[7], (D, D), D ** -0.5, 0.25)
    return dict(points=points, order=order, masks=masks, counts=counts, gain=gain, shift_bias=shift_bias, w_qkv=w_qkv, w_out=w_out)


neighbour_offsets = [(a, b, c) for a in (-1, 0, 1) for b in (-1, 0, 1) for c in (-1, 0, 1)]

def column_of(a, b, c):
    index = 9 * (a + 1) + 3 * (b + 1) + (c + 1)
    return index if index < 13 else index - 1

def layer_norm(tiled, gain, shift_bias):
    values = tiled.astype(jnp.float32)
    mean = lax.optimization_barrier(jnp.mean(values, axis=-1, keepdims=True))
    var = lax.optimization_barrier(jnp.mean((values - mean) ** 2, axis=-1, keepdims=True))
    return ((values - mean) * lax.rsqrt(var + 1e-05) * gain + shift_bias).astype(jnp.bfloat16)

def attend_slab(queries, slabs, counts_pad, masks, heads):
    by, bz, p, width = queries.shape
    hd = width // heads
    scale = 1.0 / hd ** 0.5
    positions = jnp.arange(p, dtype=jnp.int32)
    blocks = []
    valids = []
    for a, b, c in neighbour_offsets:
        block = slabs[a + 1][1 + b:1 + b + by, 1 + c:1 + c + bz]
        near = counts_pad[a + 1, 1 + b:1 + b + by, 1 + c:1 + c + bz]
        valid = positions[None, None, :] < near[:, :, None]
        if (a, b, c) != (0, 0, 0):
            valid = valid & (masks[:, :, column_of(a, b, c)][:, :, None] == 1)
        blocks.append(block)
        valids.append(valid)
    keyvals = jnp.concatenate(blocks, axis=2).reshape(by * bz, -1, 2 * width)
    valid = jnp.concatenate(valids, axis=2).reshape(by * bz, -1)
    flat_queries = queries.reshape(by * bz, p, width)

    def one_block(operands):
        query, keyval, mask = operands
        qh = query.reshape(p, heads, hd).astype(jnp.float32)
        kh = keyval[:, :width].reshape(-1, heads, hd).astype(jnp.float32)
        vh = keyval[:, width:].reshape(-1, heads, hd).astype(jnp.float32)
        scores = jnp.einsum('qhd,khd->hqk', qh, kh) * scale
        scores = jnp.where(mask[None, None, :], scores, -1e+30)
        top = lax.optimization_barrier(jnp.max(scores, axis=-1, keepdims=True))
        probs = jnp.where(mask[None, None, :], jnp.exp(scores - top), 0.0)
        total = lax.optimization_barrier(jnp.sum(probs, axis=-1))
        rounded = probs.astype(jnp.bfloat16).astype(jnp.float32)
        accum = jnp.einsum('hqk,khd->qhd', rounded, vh)
        return (accum / jnp.transpose(total)[..., None]).reshape(p, width)
    attn = lax.map(one_block, (flat_queries, keyvals, valid))
    return attn.reshape(by, bz, p, width).astype(jnp.bfloat16)

def reference(points, order, masks, counts, gain, shift_bias, w_qkv, w_out):
    nbx, by, bz, p, width = points.shape
    tiled = jnp.take_along_axis(points, order[..., None], axis=3)
    normed = layer_norm(tiled, gain, shift_bias)
    qkv = jnp.dot(normed.reshape(-1, width), w_qkv, preferred_element_type=jnp.float32).astype(jnp.bfloat16)
    qkv = qkv.reshape(nbx, by, bz, p, 3 * width)
    queries = qkv[..., :width]
    keyvals = jnp.pad(qkv[..., width:], ((1, 1), (1, 1), (1, 1), (0, 0), (0, 0)))
    counts_pad = jnp.pad(counts, 1)

    def one_slab(index):
        index = index.astype(jnp.int32)
        slab = lax.dynamic_slice_in_dim(keyvals, index, 3, 0)
        near = lax.dynamic_slice_in_dim(counts_pad, index, 3, 0)
        query = lax.dynamic_index_in_dim(queries, index, 0, keepdims=False)
        mask = lax.dynamic_index_in_dim(masks, index, 0, keepdims=False)
        return attend_slab(query, (slab[0], slab[1], slab[2]), near, mask, HEADS)
    attn = lax.map(one_slab, jnp.arange(nbx, dtype=jnp.int32))
    mixed = jnp.dot(attn.reshape(-1, width), w_out, preferred_element_type=jnp.float32).reshape(nbx, by, bz, p, width)
    mixed = tiled.astype(jnp.float32) + mixed
    live = jnp.arange(p, dtype=jnp.int32)[None, None, None, :] < counts[..., None]
    return jnp.where(live[..., None], mixed, 0.0).astype(jnp.bfloat16)
```

```python
import functools

import jax
import jax.numpy as jnp
from jax import lax
from jax.experimental import pallas as pl
from jax.experimental.pallas import tpu as pltpu
from jax.sharding import PartitionSpec as P

HEADS = 8
TILE = 256
LANES = 128
NEG = -1e30


def column_of(a, b, c):
    index = 9 * (a + 1) + 3 * (b + 1) + (c + 1)
    return index if index < 13 else index - 1


def reach(by, bz):
    spans = [(b, c) for b in (0, -1, 1) for c in (0, -1, 1)]
    return [o for o in spans if (by > 1 or o[0] == 0) and (bz > 1 or o[1] == 0)]


def prepare(pts_ref, order_ref, gain, shift, normed_ref, tiled_ref, by, bz, p):
    def one(g, carry):
        row = order_ref[0, g // bz, pl.ds(g % bz, 1), :]
        pick = lax.broadcasted_iota(jnp.int32, (p, p), 0) == row
        pick = jnp.where(pick, 1.0, 0.0).astype(jnp.bfloat16)
        tiled = lax.dot_general(
            pick, pts_ref[g], (((0,), (0,)), ((), ())), preferred_element_type=jnp.float32
        )
        if tiled_ref is not None:
            tiled_ref[g] = tiled.astype(jnp.bfloat16)
        mean = jnp.mean(tiled, axis=-1, keepdims=True)
        away = tiled - mean
        var = jnp.mean(away * away, axis=-1, keepdims=True)
        normed = away * lax.rsqrt(var + 1e-05) * gain + shift
        rows = pl.ds(pl.multiple_of(g * p, p), p)
        normed_ref[rows, :] = normed.astype(jnp.bfloat16)
        return carry

    lax.fori_loop(0, by * bz, one, 0)


def project(normed_ref, w_ref, lo, hi, put):
    for col in range(lo, hi, TILE):
        part = jnp.dot(
            normed_ref[...], w_ref[:, col : col + TILE], preferred_element_type=jnp.float32
        )
        put(col, part)


def compact(slabs, masks_ref, counts_ref, kv_ref, keep_ref, table_ref, j, l, by, bz, p):
    near = reach(by, bz)
    off = jnp.int32(0)
    slot = 0
    for s, (kind, at, present) in enumerate(slabs):
        for b, c in near:
            jj, ll = j + b, l + c
            inside = (jj >= 0) & (jj < by) & (ll >= 0) & (ll < bz) & present
            jj, ll = jnp.clip(jj, 0, by - 1), jnp.clip(ll, 0, bz - 1)
            if kind is None:
                live = inside if (b, c) == (0, 0) else inside & (
                    masks_ref[0, j, l, column_of(0, b, c)] == 1
                )
            else:
                col = jnp.where(kind, column_of(1, b, c), column_of(-1, b, c))
                live = inside & (masks_ref[0, j, l, col] == 1)
            count = jnp.where(live, counts_ref[at, jj, ll], 0)
            table_ref[0, slot] = off
            table_ref[1, slot] = off + count
            start = pl.multiple_of(off, 16)
            source = pl.multiple_of((jj * bz + ll) * p, p)

            @pl.when(count > 0)
            def _():
                keep_ref[pl.ds(start, p), :] = kv_ref[s, pl.ds(source, p), :]

            off = off + ((count + 15) // 16) * 16
            slot += 1
    return off, slot


def attend(total, slots, table_ref, keep_ref, qs_ref, m_ref, l_ref, acc_ref, width, rows):
    groups = width // TILE

    def tile(t, carry):
        base = pl.multiple_of(t * TILE, TILE)
        place = base + lax.broadcasted_iota(jnp.int32, (1, TILE), 1)
        valid = jnp.zeros((1, TILE), jnp.int32)
        for n in range(slots):
            hit = (place >= table_ref[0, n]) & (place < table_ref[1, n])
            valid = jnp.where(hit, 1, valid)
        valid = valid == 1
        for g in range(groups):
            span = slice(g * rows, (g + 1) * rows)
            keys = keep_ref[pl.ds(base, TILE), g * TILE : (g + 1) * TILE]
            values = keep_ref[pl.ds(base, TILE), width + g * TILE : width + (g + 1) * TILE]
            s = lax.dot_general(
                qs_ref[span, :], keys, (((1,), (1,)), ((), ())), preferred_element_type=jnp.float32
            )
            s = jnp.where(valid, s, NEG)
            before = m_ref[span, :]
            top = jnp.maximum(before, jnp.max(s, axis=-1, keepdims=True))
            alpha = jnp.exp(before - top)
            parts = [jnp.exp(s[:, i : i + LANES] - top) for i in range(0, TILE, LANES)]
            l_ref[span, :] = l_ref[span, :] * alpha + sum(parts[1:], parts[0])
            m_ref[span, :] = top
            weights = jnp.concatenate(parts, axis=1).astype(jnp.bfloat16)
            out = jnp.dot(weights, values, preferred_element_type=jnp.float32)
            wide = jnp.concatenate([alpha] * (TILE // LANES), axis=1)
            acc_ref[span, :] = acc_ref[span, :] * wide + out
        return carry

    lax.fori_loop(0, (total + TILE - 1) // TILE, tile, 0)


def stack_queries(q_ref, g, qs_ref, p, hd):
    per = TILE // hd
    owner = lax.broadcasted_iota(jnp.int32, (p, TILE), 1) // hd
    for h in range(HEADS):
        lo = (h // per) * TILE
        part = q_ref[g, :, lo : lo + TILE].astype(jnp.float32)
        part = jnp.where(owner == h % per, part, 0.0)
        qs_ref[h * p : (h + 1) * p, :] = part.astype(jnp.bfloat16)


def near_kernel(dims, masks_ref, counts_ref, pts_ref, order_ref, pair_ref, pair_order_ref,
                gain_ref, shift_ref, w_ref, tiled_ref, q_ref, sum_ref, ml_ref,
                normed_ref, kv_ref, keep_ref, qs_ref, m_ref, l_ref, acc_ref, table_ref):
    by, bz, p, width, n = dims
    hd = width // HEADS
    per = TILE // hd
    me = lax.axis_index("gx")
    even = me % 2 == 0
    gain, shift = gain_ref[...], shift_ref[...]
    keep_ref[...] = jnp.zeros_like(keep_ref)

    prepare(pts_ref, order_ref, gain, shift, normed_ref, tiled_ref, by, bz, p)

    def put_q(col, part):
        part = part.astype(jnp.bfloat16) * jnp.bfloat16(1.0 / hd**0.5)
        q_ref[:, :, col : col + TILE] = part.reshape(by * bz, p, TILE)

    def put_kv(s):
        def put(col, part):
            kv_ref[s, :, col - width : col - width + TILE] = part.astype(jnp.bfloat16)

        return put

    project(normed_ref, w_ref, 0, width, put_q)
    project(normed_ref, w_ref, width, 3 * width, put_kv(0))
    prepare(pair_ref, pair_order_ref, gain, shift, normed_ref, None, by, bz, p)
    project(normed_ref, w_ref, width, 3 * width, put_kv(1))

    other = jnp.where(even, me + 1, me - 1)
    present = (other >= 0) & (other < n)
    slabs = [(None, me, True), (even, jnp.clip(other, 0, n - 1), present)]
    owner = lax.broadcasted_iota(jnp.int32, (p, TILE), 1) // hd
    lane = lax.broadcasted_iota(jnp.int32, (p, LANES), 1)

    def block(g, carry):
        j, l = g // bz, g % bz
        total, slots = compact(
            slabs, masks_ref, counts_ref, kv_ref, keep_ref, table_ref, j, l, by, bz, p
        )
        stack_queries(q_ref, g, qs_ref, p, hd)
        m_ref[...] = jnp.full_like(m_ref, NEG)
        l_ref[...] = jnp.zeros_like(l_ref)
        acc_ref[...] = jnp.zeros_like(acc_ref)
        attend(total, slots, table_ref, keep_ref, qs_ref, m_ref, l_ref, acc_ref, width, per * p)
        ml = jnp.zeros((p, LANES), jnp.float32)
        for h in range(HEADS):
            rows = slice(h * p, (h + 1) * p)
            ml = jnp.where(lane == h, m_ref[rows, :], ml)
            ml = jnp.where(lane == HEADS + h, jnp.sum(l_ref[rows, :], axis=-1, keepdims=True), ml)
        ml_ref[g] = ml
        for q in range(width // TILE):
            out = jnp.zeros((p, TILE), jnp.float32)
            for h in range(per):
                rows = slice((q * per + h) * p, (q * per + h + 1) * p)
                out = jnp.where(owner == h, acc_ref[rows, :], out)
            sum_ref[g, :, q * TILE : (q + 1) * TILE] = out
        return carry

    lax.fori_loop(0, by * bz, block, 0)


def far_kernel(dims, masks_ref, counts_ref, pts_ref, order_ref, gain_ref, shift_ref, w_ref,
               w_out_ref, tiled_ref, q_ref, sum_ref, ml_ref, out_ref,
               normed_ref, kv_ref, keep_ref, qs_ref, m_ref, l_ref, acc_ref, table_ref):
    by, bz, p, width, n = dims
    hd = width // HEADS
    per = TILE // hd
    me = lax.axis_index("gx")
    even = me % 2 == 0
    keep_ref[...] = jnp.zeros_like(keep_ref)
    prepare(pts_ref, order_ref, gain_ref[...], shift_ref[...], normed_ref, None, by, bz, p)

    def put(col, part):
        kv_ref[0, :, col - width : col - width + TILE] = part.astype(jnp.bfloat16)

    project(normed_ref, w_ref, width, 3 * width, put)
    other = jnp.where(even, me - 1, me + 1)
    present = (other >= 0) & (other < n)
    slabs = [(jnp.logical_not(even), jnp.clip(other, 0, n - 1), present)]
    owner = lax.broadcasted_iota(jnp.int32, (p, TILE), 1) // hd
    lane = lax.broadcasted_iota(jnp.int32, (p, LANES), 1)

    def block(g, carry):
        j, l = g // bz, g % bz
        total, slots = compact(
            slabs, masks_ref, counts_ref, kv_ref, keep_ref, table_ref, j, l, by, bz, p
        )
        stack_queries(q_ref, g, qs_ref, p, hd)
        ml = ml_ref[g]
        for h in range(HEADS):
            rows = slice(h * p, (h + 1) * p)
            m_ref[rows, :] = jnp.broadcast_to(ml[:, h : h + 1], (p, LANES))
            l_ref[rows, :] = jnp.where(lane == HEADS + h, ml, 0.0)
            lo = (h // per) * TILE
            acc_ref[rows, :] = sum_ref[g, :, lo : lo + TILE]
        attend(total, slots, table_ref, keep_ref, qs_ref, m_ref, l_ref, acc_ref, width, per * p)
        rows_out = pl.ds(pl.multiple_of(g * p, p), p)
        for q in range(width // TILE):
            out = jnp.zeros((p, TILE), jnp.float32)
            for h in range(per):
                rows = slice((q * per + h) * p, (q * per + h + 1) * p)
                scale = 1.0 / jnp.sum(l_ref[rows, :], axis=-1, keepdims=True)
                out = jnp.where(owner == h, acc_ref[rows, :] * scale, out)
            normed_ref[rows_out, q * TILE : (q + 1) * TILE] = out.astype(jnp.bfloat16)
        return carry

    lax.fori_loop(0, by * bz, block, 0)
    row = lax.broadcasted_iota(jnp.int32, (p, TILE), 0)
    for col in range(0, width, TILE):
        mixed = jnp.dot(
            normed_ref[...], w_out_ref[:, col : col + TILE], preferred_element_type=jnp.float32
        )
        for g in range(by * bz):
            part = mixed[g * p : (g + 1) * p] + tiled_ref[g, :, col : col + TILE].astype(jnp.float32)
            part = jnp.where(row < counts_ref[me, g // bz, g % bz], part, 0.0)
            out_ref[g, :, col : col + TILE] = part.astype(jnp.bfloat16)


def shards(points, order, masks, counts, gain, shift_bias, w_qkv, w_out):
    _, by, bz, p, width = points.shape
    n = lax.axis_size("gx")
    nb = by * bz
    dims = (by, bz, p, width, n)
    pairs = [e for i in range(0, n - 1, 2) for e in ((i, i + 1), (i + 1, i))]
    across = [e for i in range(1, n - 1, 2) for e in ((i, i + 1), (i + 1, i))]
    far_order = lax.ppermute(order, "gx", across)
    far = lax.ppermute(points, "gx", across)
    pair_order = lax.ppermute(order, "gx", pairs)
    pair = lax.ppermute(points, "gx", pairs)
    flat = lambda value: value.reshape(nb, p, width)
    gain, shift = gain.reshape(1, width), shift_bias.reshape(1, width)
    smem = pl.BlockSpec(memory_space=pltpu.SMEM)
    vmem = pl.BlockSpec(memory_space=pltpu.VMEM)
    slots = len(reach(by, bz))

    def scratch(slabs):
        cap = -(-slabs * slots * p // TILE) * TILE
        return [
            pltpu.VMEM((nb * p, width), jnp.bfloat16),
            pltpu.VMEM((slabs, nb * p, 2 * width), jnp.bfloat16),
            pltpu.VMEM((cap, 2 * width), jnp.bfloat16),
            pltpu.VMEM((HEADS * p, TILE), jnp.bfloat16),
            pltpu.VMEM((HEADS * p, LANES), jnp.float32),
            pltpu.VMEM((HEADS * p, LANES), jnp.float32),
            pltpu.VMEM((HEADS * p, TILE), jnp.float32),
            pltpu.SMEM((2, slabs * slots), jnp.int32),
        ]

    shape = jax.ShapeDtypeStruct
    tiled, q, total, ml = pl.pallas_call(
        functools.partial(near_kernel, dims),
        name="near",
        out_shape=[
            shape((nb, p, width), jnp.bfloat16),
            shape((nb, p, width), jnp.bfloat16),
            shape((nb, p, width), jnp.float32),
            shape((nb, p, LANES), jnp.float32),
        ],
        in_specs=[smem, smem] + [vmem] * 7,
        out_specs=[vmem] * 4,
        scratch_shapes=scratch(2),
        cost_estimate=pl.CostEstimate(
            flops=8 * nb * p * width * 5 * width, transcendentals=0, bytes_accessed=8 << 20
        ),
        compiler_params=pltpu.CompilerParams(vmem_limit_bytes=40 << 20),
    )(masks, counts, flat(points), order, flat(pair), pair_order, gain, shift, w_qkv)
    out = pl.pallas_call(
        functools.partial(far_kernel, dims),
        name="far",
        out_shape=shape((nb, p, width), jnp.bfloat16),
        in_specs=[smem, smem] + [vmem] * 10,
        out_specs=vmem,
        scratch_shapes=scratch(1),
        cost_estimate=pl.CostEstimate(
            flops=4 * nb * p * width * 3 * width, transcendentals=0, bytes_accessed=8 << 20
        ),
        compiler_params=pltpu.CompilerParams(vmem_limit_bytes=40 << 20),
    )(masks, counts, flat(far), far_order, gain, shift, w_qkv, w_out, tiled, q, total, ml)
    return out.reshape(points.shape)


def solution(mesh):
    placed = (
        P(("groups", "gx"), None, None, None, None),
        P(("groups", "gx"), None, None, None),
        P(("groups", "gx"), None, None, None),
        P("groups", None, None),
        P(),
        P(),
        P(),
        P(),
    )
    return jax.shard_map(
        shards,
        mesh=mesh,
        in_specs=placed,
        out_specs=P(("groups", "gx"), None, None, None, None),
        check_vma=False,
    )
```

```python
import functools

import jax
import jax.numpy as jnp
from jax import lax
from jax.experimental import pallas as pl
from jax.experimental.pallas import tpu as pltpu
from jax.sharding import PartitionSpec as P

HEADS = 8
TILE = 256
LANES = 128
NEG = -1e30


def column_of(a, b, c):
    index = 9 * (a + 1) + 3 * (b + 1) + (c + 1)
    return index if index < 13 else index - 1


def reach(by, bz):
    spans = [(b, c) for b in (0, -1, 1) for c in (0, -1, 1)]
    return [o for o in spans if (by > 1 or o[0] == 0) and (bz > 1 or o[1] == 0)]


def norm_kernel(dims, pts_hbm, order_hbm, gain_hbm, shift_hbm, tiled_ref, normed_ref,
                pts_ref, order_ref, gain_ref, shift_ref, pts_sem, sems):
    by, bz, p, width, n = dims
    nb = by * bz
    smalls = [
        pltpu.make_async_copy(order_hbm, order_ref, sems.at[0]),
        pltpu.make_async_copy(gain_hbm, gain_ref, sems.at[1]),
        pltpu.make_async_copy(shift_hbm, shift_ref, sems.at[2]),
    ]
    loads = [
        pltpu.make_async_copy(pts_hbm.at[g], pts_ref.at[g], pts_sem.at[g]) for g in range(nb)
    ]
    for copy in smalls + loads:
        copy.start()
    for copy in smalls:
        copy.wait()
    for g in range(nb):
        loads[g].wait()
        row = order_ref[0, g // bz, g % bz : g % bz + 1, :]
        pick = lax.broadcasted_iota(jnp.int32, (p, p), 0) == row
        pick = jnp.where(pick, 1.0, 0.0).astype(jnp.bfloat16)
        tiled = lax.dot_general(
            pick, pts_ref[g], (((0,), (0,)), ((), ())), preferred_element_type=jnp.float32
        )
        tiled_ref[g] = tiled.astype(jnp.bfloat16)
        mean = jnp.mean(tiled, axis=-1, keepdims=True)
        away = tiled - mean
        var = jnp.mean(away * away, axis=-1, keepdims=True)
        normed = away * lax.rsqrt(var + 1e-05) * gain_ref[...] + shift_ref[...]
        normed_ref[g * p : (g + 1) * p, :] = normed.astype(jnp.bfloat16)


def project(normed_ref, w_ref, lo, hi, put):
    for col in range(lo, hi, TILE):
        part = jnp.dot(
            normed_ref[...], w_ref[:, col : col + TILE], preferred_element_type=jnp.float32
        )
        put(col, part)


def compact(slabs, masks_ref, counts_ref, kv_ref, keep_ref, table_ref, j, l, by, bz, p):
    near = reach(by, bz)
    off = jnp.int32(0)
    slot = 0
    for s, (kind, at, present) in enumerate(slabs):
        for b, c in near:
            jj, ll = j + b, l + c
            inside = (jj >= 0) & (jj < by) & (ll >= 0) & (ll < bz) & present
            jj, ll = jnp.clip(jj, 0, by - 1), jnp.clip(ll, 0, bz - 1)
            if kind is None:
                live = inside if (b, c) == (0, 0) else inside & (
                    masks_ref[0, j, l, column_of(0, b, c)] == 1
                )
            else:
                col = jnp.where(kind, column_of(1, b, c), column_of(-1, b, c))
                live = inside & (masks_ref[0, j, l, col] == 1)
            count = jnp.where(live, counts_ref[at, jj, ll], 0)
            table_ref[0, slot] = off
            table_ref[1, slot] = off + count
            start = pl.multiple_of(off, 16)
            source = pl.multiple_of((jj * bz + ll) * p, p)

            @pl.when(count > 0)
            def _():
                keep_ref[pl.ds(start, p), :] = kv_ref[s, pl.ds(source, p), :]

            off = off + ((count + 15) // 16) * 16
            slot += 1
    return off, slot


def attend(total, slots, table_ref, keep_ref, qs_ref, m_ref, l_ref, acc_ref, width, rows):
    def tile(base, span_k, first):
        place = base + lax.broadcasted_iota(jnp.int32, (1, span_k), 1)
        valid = jnp.zeros((1, span_k), jnp.int32)
        for n in range(slots):
            hit = (place >= table_ref[0, n]) & (place < table_ref[1, n])
            valid = jnp.where(hit, 1, valid)
        valid = valid == 1
        for g in range(width // TILE):
            span = slice(g * rows, (g + 1) * rows)
            keys = keep_ref[pl.ds(base, span_k), g * TILE : (g + 1) * TILE]
            values = keep_ref[pl.ds(base, span_k), width + g * TILE : width + (g + 1) * TILE]
            s = lax.dot_general(
                qs_ref[span, :], keys, (((1,), (1,)), ((), ())), preferred_element_type=jnp.float32
            )
            s = jnp.where(valid, s, NEG)
            top = jnp.max(s, axis=-1, keepdims=True)
            if first:
                top = jnp.broadcast_to(top, (rows, LANES))
            else:
                before = m_ref[span, :]
                top = jnp.maximum(before, top)
                alpha = jnp.exp(before - top)
            parts = [jnp.exp(s[:, i : i + LANES] - top) for i in range(0, span_k, LANES)]
            mass = sum(parts[1:], parts[0])
            weights = jnp.concatenate(parts, axis=1).astype(jnp.bfloat16)
            out = jnp.dot(weights, values, preferred_element_type=jnp.float32)
            m_ref[span, :] = top
            if first:
                l_ref[span, :] = mass
                acc_ref[span, :] = out
            else:
                l_ref[span, :] = l_ref[span, :] * alpha + mass
                wide = jnp.concatenate([alpha] * (TILE // LANES), axis=1)
                acc_ref[span, :] = acc_ref[span, :] * wide + out

    halves = (total + LANES - 1) // LANES
    whole = halves // 2

    @pl.when(whole > 0)
    def _():
        tile(0, TILE, True)

    @pl.when(whole == 0)
    def _():
        tile(0, LANES, True)

    def more(t, carry):
        tile(pl.multiple_of(t * TILE, TILE), TILE, False)
        return carry

    lax.fori_loop(1, whole, more, 0)

    @pl.when((whole > 0) & (halves % 2 == 1))
    def _():
        tile(pl.multiple_of(whole * TILE, TILE), LANES, False)


def stack_queries(q_ref, g, qs_ref, p, hd):
    per = TILE // hd
    owner = lax.broadcasted_iota(jnp.int32, (p, TILE), 1) // hd
    for h in range(HEADS):
        lo = (h // per) * TILE
        part = q_ref[g, :, lo : lo + TILE].astype(jnp.float32)
        part = jnp.where(owner == h % per, part, 0.0)
        qs_ref[h * p : (h + 1) * p, :] = part.astype(jnp.bfloat16)


def near_kernel(dims, masks_hbm, counts_hbm, normed_ref, pair_ref, w_hbm, q_ref, sum_ref, ml_ref,
                kv_ref, keep_ref, qs_ref, m_ref, l_ref, acc_ref, table_ref,
                masks_ref, counts_ref, w_ref, sems):
    by, bz, p, width, n = dims
    hd = width // HEADS
    per = TILE // hd
    copies = [
        pltpu.make_async_copy(w_hbm, w_ref, sems.at[0]),
        pltpu.make_async_copy(masks_hbm, masks_ref, sems.at[1]),
        pltpu.make_async_copy(counts_hbm, counts_ref, sems.at[2]),
    ]
    for copy in copies:
        copy.start()
    me = lax.axis_index("gx")
    even = me % 2 == 0
    keep_ref[...] = jnp.zeros_like(keep_ref)
    for copy in copies:
        copy.wait()

    def put_q(col, part):
        part = part.astype(jnp.bfloat16) * jnp.bfloat16(1.0 / hd**0.5)
        q_ref[:, :, col : col + TILE] = part.reshape(by * bz, p, TILE)

    def put_kv(s):
        def put(col, part):
            kv_ref[s, :, col - width : col - width + TILE] = part.astype(jnp.bfloat16)

        return put

    project(normed_ref, w_ref, 0, width, put_q)
    project(normed_ref, w_ref, width, 3 * width, put_kv(0))
    project(pair_ref, w_ref, width, 3 * width, put_kv(1))

    other = jnp.where(even, me + 1, me - 1)
    present = (other >= 0) & (other < n)
    slabs = [(None, me, True), (even, jnp.clip(other, 0, n - 1), present)]
    owner = lax.broadcasted_iota(jnp.int32, (p, TILE), 1) // hd
    lane = lax.broadcasted_iota(jnp.int32, (p, LANES), 1)

    def block(g, carry):
        j, l = g // bz, g % bz
        total, slots = compact(
            slabs, masks_ref, counts_ref, kv_ref, keep_ref, table_ref, j, l, by, bz, p
        )
        stack_queries(q_ref, g, qs_ref, p, hd)
        attend(total, slots, table_ref, keep_ref, qs_ref, m_ref, l_ref, acc_ref, width, per * p)
        ml = jnp.zeros((p, LANES), jnp.float32)
        for q in range(width // TILE):
            out = jnp.zeros((p, TILE), jnp.float32)
            for i in range(per):
                h = q * per + i
                rows = slice(h * p, (h + 1) * p)
                mass = jnp.sum(l_ref[rows, :], axis=-1, keepdims=True)
                ml = jnp.where(lane == h, m_ref[rows, :], ml)
                ml = jnp.where(lane == HEADS + h, mass, ml)
                out = jnp.where(owner == i, acc_ref[rows, :] * (1.0 / mass), out)
            sum_ref[g, :, q * TILE : (q + 1) * TILE] = out
        ml_ref[g] = ml
        return carry

    lax.fori_loop(0, by * bz, block, 0)


def far_kernel(dims, masks_hbm, counts_hbm, far_ref, w_hbm, w_out_hbm, tiled_ref, q_ref, sum_ref,
               ml_ref, out_ref, attn_ref, kv_ref, keep_ref, qs_ref, m_ref, l_ref, acc_ref, table_ref,
               masks_ref, counts_ref, w_ref, w_out_ref, sems):
    by, bz, p, width, n = dims
    hd = width // HEADS
    per = TILE // hd
    copies = [
        pltpu.make_async_copy(w_hbm.at[:, width:], w_ref, sems.at[0]),
        pltpu.make_async_copy(masks_hbm, masks_ref, sems.at[1]),
        pltpu.make_async_copy(counts_hbm, counts_ref, sems.at[2]),
        pltpu.make_async_copy(w_out_hbm, w_out_ref, sems.at[3]),
    ]
    for copy in copies:
        copy.start()
    me = lax.axis_index("gx")
    even = me % 2 == 0
    keep_ref[...] = jnp.zeros_like(keep_ref)
    for copy in copies:
        copy.wait()

    def put(col, part):
        kv_ref[0, :, col : col + TILE] = part.astype(jnp.bfloat16)

    project(far_ref, w_ref, 0, 2 * width, put)
    other = jnp.where(even, me - 1, me + 1)
    present = (other >= 0) & (other < n)
    slabs = [(jnp.logical_not(even), jnp.clip(other, 0, n - 1), present)]
    owner = lax.broadcasted_iota(jnp.int32, (p, TILE), 1) // hd

    def block(g, carry):
        j, l = g // bz, g % bz
        total, slots = compact(
            slabs, masks_ref, counts_ref, kv_ref, keep_ref, table_ref, j, l, by, bz, p
        )
        rows_out = pl.ds(pl.multiple_of(g * p, p), p)

        @pl.when(total == 0)
        def _():
            attn_ref[rows_out, :] = sum_ref[g].astype(jnp.bfloat16)

        @pl.when(total > 0)
        def _():
            stack_queries(q_ref, g, qs_ref, p, hd)
            attend(total, slots, table_ref, keep_ref, qs_ref, m_ref, l_ref, acc_ref, width, per * p)
            ml = ml_ref[g]
            for q in range(width // TILE):
                mine = jnp.zeros((p, TILE), jnp.float32)
                theirs = jnp.zeros((p, TILE), jnp.float32)
                for i in range(per):
                    h = q * per + i
                    rows = slice(h * p, (h + 1) * p)
                    top1, top2 = ml[:, h : h + 1], m_ref[rows, :]
                    top = jnp.maximum(top1, top2)
                    part1 = ml[:, HEADS + h : HEADS + h + 1] * jnp.exp(top1 - top)
                    part2 = jnp.exp(top2 - top)
                    mass = jnp.sum(l_ref[rows, :], axis=-1, keepdims=True)
                    inverse = 1.0 / (part1 + mass * part2)
                    first = jnp.concatenate([part1 * inverse] * (TILE // LANES), axis=1)
                    second = jnp.concatenate([part2 * inverse] * (TILE // LANES), axis=1)
                    mine = jnp.where(owner == i, first, mine)
                    theirs = jnp.where(owner == i, acc_ref[rows, :] * second, theirs)
                cols = slice(q * TILE, (q + 1) * TILE)
                attn_ref[rows_out, cols] = (sum_ref[g, :, cols] * mine + theirs).astype(jnp.bfloat16)

        return carry

    lax.fori_loop(0, by * bz, block, 0)
    row = lax.broadcasted_iota(jnp.int32, (p, TILE), 0)
    for col in range(0, width, TILE):
        mixed = jnp.dot(
            attn_ref[...], w_out_ref[:, col : col + TILE], preferred_element_type=jnp.float32
        )
        for g in range(by * bz):
            part = mixed[g * p : (g + 1) * p] + tiled_ref[g, :, col : col + TILE].astype(jnp.float32)
            part = jnp.where(row < counts_ref[me, g // bz, g % bz], part, 0.0)
            out_ref[g, :, col : col + TILE] = part.astype(jnp.bfloat16)


def shards(points, order, masks, counts, gain, shift_bias, w_qkv, w_out):
    _, by, bz, p, width = points.shape
    n = lax.axis_size("gx")
    nb = by * bz
    dims = (by, bz, p, width, n)
    pairs = [e for i in range(0, n - 1, 2) for e in ((i, i + 1), (i + 1, i))]
    across = [e for i in range(1, n - 1, 2) for e in ((i, i + 1), (i + 1, i))]
    pin = lambda value: pltpu.with_memory_space_constraint(value, pltpu.HBM)
    masks, counts, w_qkv, w_out = pin(masks), pin(counts), pin(w_qkv), pin(w_out)
    shape = jax.ShapeDtypeStruct
    dma = pltpu.SemaphoreType.DMA
    vmem = pl.BlockSpec(memory_space=pltpu.VMEM)
    hbm = pl.BlockSpec(memory_space=pltpu.HBM)
    tiled, normed = pl.pallas_call(
        functools.partial(norm_kernel, dims),
        name="norm",
        out_shape=[shape((nb, p, width), jnp.bfloat16), shape((nb * p, width), jnp.bfloat16)],
        in_specs=[hbm] * 4,
        out_specs=[vmem] * 2,
        scratch_shapes=[
            pltpu.VMEM((nb, p, width), jnp.bfloat16),
            pltpu.VMEM(order.shape, jnp.int32),
            pltpu.VMEM((1, width), jnp.float32),
            pltpu.VMEM((1, width), jnp.float32),
            dma((nb,)),
            dma((3,)),
        ],
        cost_estimate=pl.CostEstimate(
            flops=2 * nb * p * p * width, transcendentals=0, bytes_accessed=2 << 20
        ),
        compiler_params=pltpu.CompilerParams(vmem_limit_bytes=24 << 20),
    )(
        pin(points.reshape(nb, p, width)),
        pin(order),
        pin(gain.reshape(1, width)),
        pin(shift_bias.reshape(1, width)),
    )
    far = lax.ppermute(normed, "gx", across)
    pair = lax.ppermute(normed, "gx", pairs)
    slots = len(reach(by, bz))

    def scratch(slabs):
        cap = -(-slabs * slots * p // TILE) * TILE
        return [
            pltpu.VMEM((slabs, nb * p, 2 * width), jnp.bfloat16),
            pltpu.VMEM((cap, 2 * width), jnp.bfloat16),
            pltpu.VMEM((HEADS * p, TILE), jnp.bfloat16),
            pltpu.VMEM((HEADS * p, LANES), jnp.float32),
            pltpu.VMEM((HEADS * p, LANES), jnp.float32),
            pltpu.VMEM((HEADS * p, TILE), jnp.float32),
            pltpu.SMEM((2, slabs * slots), jnp.int32),
            pltpu.SMEM(masks.shape, jnp.int32),
            pltpu.SMEM(counts.shape, jnp.int32),
        ]

    q, total, ml = pl.pallas_call(
        functools.partial(near_kernel, dims),
        name="near",
        out_shape=[
            shape((nb, p, width), jnp.bfloat16),
            shape((nb, p, width), jnp.float32),
            shape((nb, p, LANES), jnp.float32),
        ],
        in_specs=[hbm, hbm, vmem, vmem, hbm],
        out_specs=[vmem] * 3,
        scratch_shapes=scratch(2) + [pltpu.VMEM(w_qkv.shape, jnp.bfloat16), dma((3,))],
        cost_estimate=pl.CostEstimate(
            flops=8 * nb * p * width * 5 * width, transcendentals=0, bytes_accessed=8 << 20
        ),
        compiler_params=pltpu.CompilerParams(vmem_limit_bytes=40 << 20),
    )(masks, counts, normed, pair, w_qkv)
    out = pl.pallas_call(
        functools.partial(far_kernel, dims),
        name="far",
        out_shape=shape((nb, p, width), jnp.bfloat16),
        in_specs=[hbm, hbm, vmem, hbm, hbm] + [vmem] * 4,
        out_specs=vmem,
        scratch_shapes=[pltpu.VMEM((nb * p, width), jnp.bfloat16)]
        + scratch(1)
        + [
            pltpu.VMEM((width, 2 * width), jnp.bfloat16),
            pltpu.VMEM((width, width), jnp.bfloat16),
            dma((4,)),
        ],
        cost_estimate=pl.CostEstimate(
            flops=4 * nb * p * width * 3 * width, transcendentals=0, bytes_accessed=8 << 20
        ),
        compiler_params=pltpu.CompilerParams(vmem_limit_bytes=40 << 20),
    )(masks, counts, far, w_qkv, w_out, tiled, q, total, ml)
    return out.reshape(points.shape)


def solution(mesh):
    placed = (
        P(("groups", "gx"), None, None, None, None),
        P(("groups", "gx"), None, None, None),
        P(("groups", "gx"), None, None, None),
        P("groups", None, None),
        P(),
        P(),
        P(),
        P(),
    )
    return jax.shard_map(
        shards,
        mesh=mesh,
        in_specs=placed,
        out_specs=P(("groups", "gx"), None, None, None, None),
        check_vma=False,
    )
```

```python
import functools

import jax
import jax.numpy as jnp
from jax import lax
from jax.experimental import pallas as pl
from jax.experimental.pallas import tpu as pltpu
from jax.sharding import PartitionSpec as P

HEADS = 8
TILE = 256
LANES = 128
NEG = -1e30


def column_of(a, b, c):
    index = 9 * (a + 1) + 3 * (b + 1) + (c + 1)
    return index if index < 13 else index - 1


def reach(by, bz):
    spans = [(b, c) for b in (0, -1, 1) for c in (0, -1, 1)]
    return [o for o in spans if (by > 1 or o[0] == 0) and (bz > 1 or o[1] == 0)]


def norm_kernel(dims, pts_hbm, order_hbm, gain_hbm, shift_hbm, tiled_ref, normed_ref,
                pts_ref, order_ref, gain_ref, shift_ref, pts_sem, sems):
    by, bz, p, width, n = dims
    nb = by * bz
    smalls = [
        pltpu.make_async_copy(order_hbm, order_ref, sems.at[0]),
        pltpu.make_async_copy(gain_hbm, gain_ref, sems.at[1]),
        pltpu.make_async_copy(shift_hbm, shift_ref, sems.at[2]),
    ]
    loads = [
        pltpu.make_async_copy(pts_hbm.at[g], pts_ref.at[g], pts_sem.at[g]) for g in range(nb)
    ]
    for copy in smalls + loads:
        copy.start()
    for copy in smalls:
        copy.wait()
    for g in range(nb):
        loads[g].wait()
        row = order_ref[0, g // bz, g % bz : g % bz + 1, :]
        pick = lax.broadcasted_iota(jnp.int32, (p, p), 0) == row
        pick = jnp.where(pick, 1.0, 0.0).astype(jnp.bfloat16)
        tiled = lax.dot_general(
            pick, pts_ref[g], (((0,), (0,)), ((), ())), preferred_element_type=jnp.float32
        )
        tiled_ref[g] = tiled.astype(jnp.bfloat16)
        mean = jnp.mean(tiled, axis=-1, keepdims=True)
        away = tiled - mean
        var = jnp.mean(away * away, axis=-1, keepdims=True)
        normed = away * lax.rsqrt(var + 1e-05) * gain_ref[...] + shift_ref[...]
        normed_ref[g * p : (g + 1) * p, :] = normed.astype(jnp.bfloat16)


def project(normed_ref, w_ref, lo, hi, put):
    for col in range(lo, hi, TILE):
        part = jnp.dot(
            normed_ref[...], w_ref[:, col : col + TILE], preferred_element_type=jnp.float32
        )
        put(col, part)


def compact(slabs, masks_ref, counts_ref, kv_ref, keep_ref, table_ref, j, l, by, bz, p):
    near = reach(by, bz)
    off = jnp.int32(0)
    slot = 0
    for s, (kind, at, present) in enumerate(slabs):
        for b, c in near:
            jj, ll = j + b, l + c
            inside = (jj >= 0) & (jj < by) & (ll >= 0) & (ll < bz) & present
            jj, ll = jnp.clip(jj, 0, by - 1), jnp.clip(ll, 0, bz - 1)
            if kind is None:
                live = inside if (b, c) == (0, 0) else inside & (
                    masks_ref[0, j, l, column_of(0, b, c)] == 1
                )
            else:
                col = jnp.where(kind, column_of(1, b, c), column_of(-1, b, c))
                live = inside & (masks_ref[0, j, l, col] == 1)
            count = jnp.where(live, counts_ref[at, jj * bz + ll], 0)
            table_ref[0, slot] = off
            table_ref[1, slot] = off + count
            start = pl.multiple_of(off, 16)
            source = pl.multiple_of((jj * bz + ll) * p, p)

            @pl.when(count > 0)
            def _():
                keep_ref[pl.ds(start, p), :] = kv_ref[s, pl.ds(source, p), :]

            off = off + ((count + 15) // 16) * 16
            slot += 1
    return off, slot


def attend(total, slots, table_ref, keep_ref, qs_ref, m_ref, l_ref, acc_ref, spare, width, hd, r):
    per = TILE // hd
    owner = lax.broadcasted_iota(jnp.int32, (r, TILE), 1) // hd
    lane = lax.broadcasted_iota(jnp.int32, (r, LANES), 1)

    def tile(base, span_k, m_ref, l_ref, acc_ref):
        place = base + lax.broadcasted_iota(jnp.int32, (1, span_k), 1)
        valid = jnp.zeros((1, span_k), jnp.int32)
        for n in range(slots):
            hit = (place >= table_ref[0, n]) & (place < table_ref[1, n])
            valid = jnp.where(hit, 1, valid)
        valid = valid == 1
        tops = jnp.zeros((r, LANES), jnp.float32)
        sums = jnp.ones((r, LANES), jnp.float32)
        for g in range(width // TILE):
            cols = slice(g * TILE, (g + 1) * TILE)
            keys = keep_ref[pl.ds(base, span_k), cols]
            values = keep_ref[pl.ds(base, span_k), width + g * TILE : width + (g + 1) * TILE]
            s = lax.dot_general(
                qs_ref[g * per * r : (g + 1) * per * r, :],
                keys,
                (((1,), (1,)), ((), ())),
                preferred_element_type=jnp.float32,
            )
            weights = []
            for i in range(per):
                h = g * per + i
                part = jnp.where(valid, s[i * r : (i + 1) * r], NEG)
                top = jnp.max(part, axis=-1, keepdims=True)
                part = jnp.exp(part - top)
                mass = jnp.sum(part, axis=-1, keepdims=True)
                tops = jnp.where(lane == h, top, tops)
                sums = jnp.where(lane == h, mass, sums)
                weights.append(part.astype(jnp.bfloat16))
            weights = jnp.concatenate(weights, axis=0)
            out = jnp.dot(weights, values, preferred_element_type=jnp.float32)
            packed = out[:r]
            for i in range(1, per):
                packed = jnp.where(owner == i, out[i * r : (i + 1) * r], packed)
            acc_ref[:r, cols] = packed
        m_ref[:r, :] = tops
        l_ref[:r, :] = sums

    def merge():
        m2_ref, l2_ref, acc2_ref = spare
        top = jnp.maximum(m_ref[:r, :], m2_ref[:r, :])
        part1 = jnp.exp(m_ref[:r, :] - top)
        part2 = jnp.exp(m2_ref[:r, :] - top)
        m_ref[:r, :] = top
        l_ref[:r, :] = l_ref[:r, :] * part1 + l2_ref[:r, :] * part2
        for g in range(width // TILE):
            cols = slice(g * TILE, (g + 1) * TILE)
            both = acc_ref[:r, cols] * spread(part1, owner, g, per, r)
            acc_ref[:r, cols] = both + acc2_ref[:r, cols] * spread(part2, owner, g, per, r)

    halves = (total + LANES - 1) // LANES
    whole = halves // 2

    @pl.when(whole > 0)
    def _():
        tile(0, TILE, m_ref, l_ref, acc_ref)

    @pl.when(whole == 0)
    def _():
        tile(0, LANES, m_ref, l_ref, acc_ref)

    def more(t, carry):
        @pl.when(t < whole)
        def _():
            tile(pl.multiple_of(t * TILE, TILE), TILE, *spare)

        @pl.when(t == whole)
        def _():
            tile(pl.multiple_of(t * TILE, TILE), LANES, *spare)

        merge()
        return carry

    lax.fori_loop(1, (halves + 1) // 2, more, 0)


def spread(packed, owner, g, per, r):
    out = jnp.zeros((r, TILE), jnp.float32)
    for i in range(per):
        out = jnp.where(owner == i, packed[:, g * per + i : g * per + i + 1], out)
    return out


def stack_queries(q_ref, g, qs_ref, hd, r):
    per = TILE // hd
    owner = lax.broadcasted_iota(jnp.int32, (r, TILE), 1) // hd
    for h in range(HEADS):
        lo = (h // per) * TILE
        part = q_ref[g, :r, lo : lo + TILE].astype(jnp.float32)
        part = jnp.where(owner == h % per, part, 0.0)
        qs_ref[h * r : (h + 1) * r, :] = part.astype(jnp.bfloat16)


def by_rows(live, p, body):
    half = p // 2

    @pl.when(live <= half)
    def _():
        body(half)

    @pl.when(live > half)
    def _():
        body(p)


def near_kernel(dims, masks_hbm, counts_hbm, normed_ref, pair_ref, w_hbm, q_ref, sum_ref, m_ref,
                l_ref, kv_ref, keep_ref, qs_ref, table_ref, masks_ref, counts_ref, m2_ref, l2_ref,
                acc2_ref, w_ref, sems):
    by, bz, p, width, n = dims
    hd = width // HEADS
    per = TILE // hd
    copies = [
        pltpu.make_async_copy(w_hbm, w_ref, sems.at[0]),
        pltpu.make_async_copy(masks_hbm, masks_ref, sems.at[1]),
        pltpu.make_async_copy(counts_hbm, counts_ref, sems.at[2]),
    ]
    for copy in copies:
        copy.start()
    me = lax.axis_index("gx")
    even = me % 2 == 0
    keep_ref[...] = jnp.zeros_like(keep_ref)
    for copy in copies:
        copy.wait()

    def put_q(col, part):
        part = part.astype(jnp.bfloat16) * jnp.bfloat16(1.0 / hd**0.5)
        q_ref[:, :, col : col + TILE] = part.reshape(by * bz, p, TILE)

    def put_kv(s):
        def put(col, part):
            kv_ref[s, :, col - width : col - width + TILE] = part.astype(jnp.bfloat16)

        return put

    project(normed_ref, w_ref, 0, width, put_q)
    project(normed_ref, w_ref, width, 3 * width, put_kv(0))
    project(pair_ref, w_ref, width, 3 * width, put_kv(1))

    other = jnp.where(even, me + 1, me - 1)
    present = (other >= 0) & (other < n)
    slabs = [(None, me, True), (even, jnp.clip(other, 0, n - 1), present)]

    def block(g, carry):
        j, l = g // bz, g % bz
        total, slots = compact(
            slabs, masks_ref, counts_ref, kv_ref, keep_ref, table_ref, j, l, by, bz, p
        )

        def rows(r):
            stack_queries(q_ref, g, qs_ref, hd, r)
            attend(
                total, slots, table_ref, keep_ref, qs_ref,
                m_ref.at[g], l_ref.at[g], sum_ref.at[g], (m2_ref, l2_ref, acc2_ref), width, hd, r,
            )
            owner = lax.broadcasted_iota(jnp.int32, (r, TILE), 1) // hd
            inverse = 1.0 / l_ref[g, :r, :]
            for q in range(width // TILE):
                cols = slice(q * TILE, (q + 1) * TILE)
                sum_ref[g, :r, cols] = sum_ref[g, :r, cols] * spread(inverse, owner, q, per, r)

        by_rows(counts_ref[me, g], p, rows)
        return carry

    lax.fori_loop(0, by * bz, block, 0)


def far_kernel(dims, masks_hbm, counts_hbm, far_ref, w_hbm, w_out_hbm, tiled_ref, q_ref, sum_ref,
               near_m_ref, near_l_ref, out_ref, attn_ref, kv_ref, keep_ref, qs_ref, table_ref,
               masks_ref, counts_ref, m2_ref, l2_ref, acc2_ref, m_ref, l_ref, acc_ref, w_ref, w_out_ref, sems):
    by, bz, p, width, n = dims
    hd = width // HEADS
    per = TILE // hd
    copies = [
        pltpu.make_async_copy(w_hbm.at[:, width:], w_ref, sems.at[0]),
        pltpu.make_async_copy(masks_hbm, masks_ref, sems.at[1]),
        pltpu.make_async_copy(counts_hbm, counts_ref, sems.at[2]),
        pltpu.make_async_copy(w_out_hbm, w_out_ref, sems.at[3]),
    ]
    for copy in copies:
        copy.start()
    me = lax.axis_index("gx")
    even = me % 2 == 0
    keep_ref[...] = jnp.zeros_like(keep_ref)
    for copy in copies:
        copy.wait()

    def put(col, part):
        kv_ref[0, :, col : col + TILE] = part.astype(jnp.bfloat16)

    project(far_ref, w_ref, 0, 2 * width, put)
    other = jnp.where(even, me - 1, me + 1)
    present = (other >= 0) & (other < n)
    slabs = [(jnp.logical_not(even), jnp.clip(other, 0, n - 1), present)]

    def block(g, carry):
        j, l = g // bz, g % bz
        total, slots = compact(
            slabs, masks_ref, counts_ref, kv_ref, keep_ref, table_ref, j, l, by, bz, p
        )
        rows_out = pl.ds(pl.multiple_of(g * p, p), p)

        @pl.when(total == 0)
        def _():
            attn_ref[rows_out, :] = sum_ref[g].astype(jnp.bfloat16)

        def rows(r):
            stack_queries(q_ref, g, qs_ref, hd, r)
            attend(
                total, slots, table_ref, keep_ref, qs_ref, m_ref, l_ref, acc_ref,
                (m2_ref, l2_ref, acc2_ref), width, hd, r,
            )
            owner = lax.broadcasted_iota(jnp.int32, (r, TILE), 1) // hd
            top1, top2 = near_m_ref[g, :r, :], m_ref[:r, :]
            top = jnp.maximum(top1, top2)
            part1 = near_l_ref[g, :r, :] * jnp.exp(top1 - top)
            part2 = jnp.exp(top2 - top)
            inverse = 1.0 / (part1 + l_ref[:r, :] * part2)
            part1, part2 = part1 * inverse, part2 * inverse
            some = pl.ds(pl.multiple_of(g * p, p), r)
            for q in range(width // TILE):
                cols = slice(q * TILE, (q + 1) * TILE)
                mixed = sum_ref[g, :r, cols] * spread(part1, owner, q, per, r)
                mixed = mixed + acc_ref[:r, cols] * spread(part2, owner, q, per, r)
                attn_ref[some, cols] = mixed.astype(jnp.bfloat16)

        @pl.when(total > 0)
        def _():
            by_rows(counts_ref[me, g], p, rows)

        return carry

    lax.fori_loop(0, by * bz, block, 0)
    row = lax.broadcasted_iota(jnp.int32, (p, TILE), 0)
    for col in range(0, width, TILE):
        mixed = jnp.dot(
            attn_ref[...], w_out_ref[:, col : col + TILE], preferred_element_type=jnp.float32
        )
        for g in range(by * bz):
            part = mixed[g * p : (g + 1) * p] + tiled_ref[g, :, col : col + TILE].astype(jnp.float32)
            part = jnp.where(row < counts_ref[me, g], part, 0.0)
            out_ref[g, :, col : col + TILE] = part.astype(jnp.bfloat16)


def shards(points, order, masks, counts, gain, shift_bias, w_qkv, w_out):
    _, by, bz, p, width = points.shape
    n = lax.axis_size("gx")
    nb = by * bz
    dims = (by, bz, p, width, n)
    pairs = [e for i in range(0, n - 1, 2) for e in ((i, i + 1), (i + 1, i))]
    across = [e for i in range(1, n - 1, 2) for e in ((i, i + 1), (i + 1, i))]
    counts = counts.reshape(counts.shape[0], nb)
    pin = lambda value: pltpu.with_memory_space_constraint(value, pltpu.HBM)
    masks, counts, w_qkv, w_out = pin(masks), pin(counts), pin(w_qkv), pin(w_out)
    shape = jax.ShapeDtypeStruct
    dma = pltpu.SemaphoreType.DMA
    vmem = pl.BlockSpec(memory_space=pltpu.VMEM)
    hbm = pl.BlockSpec(memory_space=pltpu.HBM)
    tiled, normed = pl.pallas_call(
        functools.partial(norm_kernel, dims),
        name="norm",
        out_shape=[shape((nb, p, width), jnp.bfloat16), shape((nb * p, width), jnp.bfloat16)],
        in_specs=[hbm] * 4,
        out_specs=[vmem] * 2,
        scratch_shapes=[
            pltpu.VMEM((nb, p, width), jnp.bfloat16),
            pltpu.VMEM(order.shape, jnp.int32),
            pltpu.VMEM((1, width), jnp.float32),
            pltpu.VMEM((1, width), jnp.float32),
            dma((nb,)),
            dma((3,)),
        ],
        cost_estimate=pl.CostEstimate(
            flops=2 * nb * p * p * width, transcendentals=0, bytes_accessed=2 << 20
        ),
        compiler_params=pltpu.CompilerParams(vmem_limit_bytes=24 << 20),
    )(
        pin(points.reshape(nb, p, width)),
        pin(order),
        pin(gain.reshape(1, width)),
        pin(shift_bias.reshape(1, width)),
    )
    far = lax.ppermute(normed, "gx", across)
    pair = lax.ppermute(normed, "gx", pairs)
    slots = len(reach(by, bz))

    def scratch(slabs):
        cap = -(-slabs * slots * p // TILE) * TILE
        return [
            pltpu.VMEM((slabs, nb * p, 2 * width), jnp.bfloat16),
            pltpu.VMEM((cap, 2 * width), jnp.bfloat16),
            pltpu.VMEM((HEADS * p, TILE), jnp.bfloat16),
            pltpu.SMEM((2, slabs * slots), jnp.int32),
            pltpu.SMEM(masks.shape, jnp.int32),
            pltpu.SMEM(counts.shape, jnp.int32),
            pltpu.VMEM((p, LANES), jnp.float32),
            pltpu.VMEM((p, LANES), jnp.float32),
            pltpu.VMEM((p, width), jnp.float32),
        ]

    q, total, tops, sums = pl.pallas_call(
        functools.partial(near_kernel, dims),
        name="near",
        out_shape=[
            shape((nb, p, width), jnp.bfloat16),
            shape((nb, p, width), jnp.float32),
            shape((nb, p, LANES), jnp.float32),
            shape((nb, p, LANES), jnp.float32),
        ],
        in_specs=[hbm, hbm, vmem, vmem, hbm],
        out_specs=[vmem] * 4,
        scratch_shapes=scratch(2) + [pltpu.VMEM(w_qkv.shape, jnp.bfloat16), dma((3,))],
        cost_estimate=pl.CostEstimate(
            flops=8 * nb * p * width * 5 * width, transcendentals=0, bytes_accessed=8 << 20
        ),
        compiler_params=pltpu.CompilerParams(vmem_limit_bytes=40 << 20),
    )(masks, counts, normed, pair, w_qkv)
    out = pl.pallas_call(
        functools.partial(far_kernel, dims),
        name="far",
        out_shape=shape((nb, p, width), jnp.bfloat16),
        in_specs=[hbm, hbm, vmem, hbm, hbm] + [vmem] * 5,
        out_specs=vmem,
        scratch_shapes=[pltpu.VMEM((nb * p, width), jnp.bfloat16)]
        + scratch(1)
        + [
            pltpu.VMEM((p, LANES), jnp.float32),
            pltpu.VMEM((p, LANES), jnp.float32),
            pltpu.VMEM((p, width), jnp.float32),
            pltpu.VMEM((width, 2 * width), jnp.bfloat16),
            pltpu.VMEM((width, width), jnp.bfloat16),
            dma((4,)),
        ],
        cost_estimate=pl.CostEstimate(
            flops=4 * nb * p * width * 3 * width, transcendentals=0, bytes_accessed=8 << 20
        ),
        compiler_params=pltpu.CompilerParams(vmem_limit_bytes=40 << 20),
    )(masks, counts, far, w_qkv, w_out, tiled, q, total, tops, sums)
    return out.reshape(points.shape)


def solution(mesh):
    placed = (
        P(("groups", "gx"), None, None, None, None),
        P(("groups", "gx"), None, None, None),
        P(("groups", "gx"), None, None, None),
        P("groups", None, None),
        P(),
        P(),
        P(),
        P(),
    )
    return jax.shard_map(
        shards,
        mesh=mesh,
        in_specs=placed,
        out_specs=P(("groups", "gx"), None, None, None, None),
        check_vma=False,
    )
```

```python
import functools

import jax
import jax.numpy as jnp
from jax import lax
from jax.experimental import pallas as pl
from jax.experimental.pallas import tpu as pltpu
from jax.sharding import PartitionSpec as P

HEADS = 8
TILE = 256
LANES = 128
NEG = -1e30


def column_of(a, b, c):
    index = 9 * (a + 1) + 3 * (b + 1) + (c + 1)
    return index if index < 13 else index - 1


def reach(by, bz):
    spans = [(b, c) for b in (0, -1, 1) for c in (0, -1, 1)]
    return [o for o in spans if (by > 1 or o[0] == 0) and (bz > 1 or o[1] == 0)]


def norm_kernel(dims, pts_hbm, order_hbm, gain_hbm, shift_hbm, tiled_ref, normed_ref,
                pts_ref, order_ref, gain_ref, shift_ref, pts_sem, sems):
    by, bz, p, width, n = dims
    nb = by * bz
    smalls = [
        pltpu.make_async_copy(order_hbm, order_ref, sems.at[0]),
        pltpu.make_async_copy(gain_hbm, gain_ref, sems.at[1]),
        pltpu.make_async_copy(shift_hbm, shift_ref, sems.at[2]),
    ]
    loads = [
        pltpu.make_async_copy(pts_hbm.at[g], pts_ref.at[g], pts_sem.at[g]) for g in range(nb)
    ]
    for copy in smalls + loads:
        copy.start()
    for copy in smalls:
        copy.wait()
    for g in range(nb):
        loads[g].wait()
        row = order_ref[0, g // bz, g % bz : g % bz + 1, :]
        pick = lax.broadcasted_iota(jnp.int32, (p, p), 0) == row
        pick = jnp.where(pick, 1.0, 0.0).astype(jnp.bfloat16)
        tiled = lax.dot_general(
            pick, pts_ref[g], (((0,), (0,)), ((), ())), preferred_element_type=jnp.float32
        )
        tiled_ref[g] = tiled.astype(jnp.bfloat16)
        mean = jnp.mean(tiled, axis=-1, keepdims=True)
        away = tiled - mean
        var = jnp.mean(away * away, axis=-1, keepdims=True)
        normed = away * lax.rsqrt(var + 1e-05) * gain_ref[...] + shift_ref[...]
        normed_ref[g * p : (g + 1) * p, :] = normed.astype(jnp.bfloat16)


def project(normed_ref, w_ref, lo, hi, put):
    for col in range(lo, hi, TILE):
        part = jnp.dot(
            normed_ref[...], w_ref[:, col : col + TILE], preferred_element_type=jnp.float32
        )
        put(col, part)


def compact(slabs, masks_ref, counts_ref, kv_ref, keep_ref, table_ref, j, l, by, bz, p):
    near = reach(by, bz)
    off = jnp.int32(0)
    slot = 0
    for s, (kind, at, present) in enumerate(slabs):
        for b, c in near:
            jj, ll = j + b, l + c
            inside = (jj >= 0) & (jj < by) & (ll >= 0) & (ll < bz) & present
            jj, ll = jnp.clip(jj, 0, by - 1), jnp.clip(ll, 0, bz - 1)
            if kind is None:
                live = inside if (b, c) == (0, 0) else inside & (
                    masks_ref[0, j, l, column_of(0, b, c)] == 1
                )
            else:
                col = jnp.where(kind, column_of(1, b, c), column_of(-1, b, c))
                live = inside & (masks_ref[0, j, l, col] == 1)
            count = jnp.where(live, counts_ref[at, jj * bz + ll], 0)
            table_ref[0, slot] = off
            table_ref[1, slot] = off + count
            start = pl.multiple_of(off, 16)
            source = pl.multiple_of((jj * bz + ll) * p, p)

            @pl.when(count > 0)
            def _():
                keep_ref[pl.ds(start, p), :] = kv_ref[s, pl.ds(source, p), :]

            off = off + ((count + 15) // 16) * 16
            slot += 1
    return off, slot


def attend(total, slots, table_ref, keep_ref, qs_ref, m_ref, l_ref, acc_ref, spare, width, hd, r):
    per = TILE // hd
    owner = lax.broadcasted_iota(jnp.int32, (r, TILE), 1) // hd
    lane = lax.broadcasted_iota(jnp.int32, (r, LANES), 1)

    def tile(base, span_k, m_ref, l_ref, acc_ref):
        place = base + lax.broadcasted_iota(jnp.int32, (1, span_k), 1)
        valid = jnp.zeros((1, span_k), jnp.int32)
        for n in range(slots):
            hit = (place >= table_ref[0, n]) & (place < table_ref[1, n])
            valid = jnp.where(hit, 1, valid)
        valid = valid == 1
        tops = jnp.zeros((r, LANES), jnp.float32)
        sums = jnp.ones((r, LANES), jnp.float32)
        for g in range(width // TILE):
            cols = slice(g * TILE, (g + 1) * TILE)
            keys = keep_ref[pl.ds(base, span_k), cols]
            values = keep_ref[pl.ds(base, span_k), width + g * TILE : width + (g + 1) * TILE]
            s = lax.dot_general(
                qs_ref[g * per * r : (g + 1) * per * r, :],
                keys,
                (((1,), (1,)), ((), ())),
                preferred_element_type=jnp.float32,
            )
            weights = []
            for i in range(per):
                h = g * per + i
                part = jnp.where(valid, s[i * r : (i + 1) * r], NEG)
                top = jnp.max(part, axis=-1, keepdims=True)
                part = jnp.exp(part - top)
                mass = jnp.sum(part, axis=-1, keepdims=True)
                tops = jnp.where(lane == h, top, tops)
                sums = jnp.where(lane == h, mass, sums)
                weights.append(part.astype(jnp.bfloat16))
            weights = jnp.concatenate(weights, axis=0)
            out = jnp.dot(weights, values, preferred_element_type=jnp.float32)
            packed = out[:r]
            for i in range(1, per):
                packed = jnp.where(owner == i, out[i * r : (i + 1) * r], packed)
            acc_ref[:r, cols] = packed
        m_ref[:r, :] = tops
        l_ref[:r, :] = sums

    def merge():
        m2_ref, l2_ref, acc2_ref = spare
        top = jnp.maximum(m_ref[:r, :], m2_ref[:r, :])
        part1 = jnp.exp(m_ref[:r, :] - top)
        part2 = jnp.exp(m2_ref[:r, :] - top)
        m_ref[:r, :] = top
        l_ref[:r, :] = l_ref[:r, :] * part1 + l2_ref[:r, :] * part2
        for g in range(width // TILE):
            cols = slice(g * TILE, (g + 1) * TILE)
            both = acc_ref[:r, cols] * spread(part1, owner, g, per, r)
            acc_ref[:r, cols] = both + acc2_ref[:r, cols] * spread(part2, owner, g, per, r)

    halves = (total + LANES - 1) // LANES
    whole = halves // 2

    @pl.when(whole > 0)
    def _():
        tile(0, TILE, m_ref, l_ref, acc_ref)

    @pl.when(whole == 0)
    def _():
        tile(0, LANES, m_ref, l_ref, acc_ref)

    def more(t, carry):
        @pl.when(t < whole)
        def _():
            tile(pl.multiple_of(t * TILE, TILE), TILE, *spare)

        @pl.when(t == whole)
        def _():
            tile(pl.multiple_of(t * TILE, TILE), LANES, *spare)

        merge()
        return carry

    lax.fori_loop(1, (halves + 1) // 2, more, 0)


def spread(packed, owner, g, per, r):
    out = jnp.zeros((r, TILE), jnp.float32)
    for i in range(per):
        out = jnp.where(owner == i, packed[:, g * per + i : g * per + i + 1], out)
    return out


def stack_queries(q_ref, g, qs_ref, hd, r):
    per = TILE // hd
    owner = lax.broadcasted_iota(jnp.int32, (r, TILE), 1) // hd
    for h in range(HEADS):
        lo = (h // per) * TILE
        part = q_ref[g, :r, lo : lo + TILE].astype(jnp.float32)
        part = jnp.where(owner == h % per, part, 0.0)
        qs_ref[h * r : (h + 1) * r, :] = part.astype(jnp.bfloat16)


def by_rows(live, p, body):
    half = p // 2

    @pl.when(live <= half)
    def _():
        body(half)

    @pl.when(live > half)
    def _():
        body(p)


def near_kernel(dims, masks_hbm, counts_hbm, normed_ref, pair_ref, w_hbm, q_ref, sum_ref, m_ref,
                l_ref, kv_ref, keep_ref, qs_ref, table_ref, masks_ref, counts_ref, m2_ref, l2_ref,
                acc2_ref, w_ref, sems):
    by, bz, p, width, n = dims
    hd = width // HEADS
    per = TILE // hd
    copies = [
        pltpu.make_async_copy(w_hbm, w_ref, sems.at[0]),
        pltpu.make_async_copy(masks_hbm, masks_ref, sems.at[1]),
        pltpu.make_async_copy(counts_hbm, counts_ref, sems.at[2]),
    ]
    for copy in copies:
        copy.start()
    me = lax.axis_index("gx")
    even = me % 2 == 0
    keep_ref[...] = jnp.zeros_like(keep_ref)
    copies[0].wait()

    def put_q(col, part):
        part = part.astype(jnp.bfloat16) * jnp.bfloat16(1.0 / hd**0.5)
        q_ref[:, :, col : col + TILE] = part.reshape(by * bz, p, TILE)

    def put_kv(s):
        def put(col, part):
            kv_ref[s, :, col - width : col - width + TILE] = part.astype(jnp.bfloat16)

        return put

    project(normed_ref, w_ref, 0, width, put_q)
    project(normed_ref, w_ref, width, 3 * width, put_kv(0))
    project(pair_ref, w_ref, width, 3 * width, put_kv(1))
    for copy in copies[1:]:
        copy.wait()

    other = jnp.where(even, me + 1, me - 1)
    present = (other >= 0) & (other < n)
    slabs = [(None, me, True), (even, jnp.clip(other, 0, n - 1), present)]

    def block(g, carry):
        j, l = g // bz, g % bz
        total, slots = compact(
            slabs, masks_ref, counts_ref, kv_ref, keep_ref, table_ref, j, l, by, bz, p
        )

        def rows(r):
            stack_queries(q_ref, g, qs_ref, hd, r)
            attend(
                total, slots, table_ref, keep_ref, qs_ref,
                m_ref.at[g], l_ref.at[g], sum_ref.at[g], (m2_ref, l2_ref, acc2_ref), width, hd, r,
            )
            owner = lax.broadcasted_iota(jnp.int32, (r, TILE), 1) // hd
            inverse = 1.0 / l_ref[g, :r, :]
            for q in range(width // TILE):
                cols = slice(q * TILE, (q + 1) * TILE)
                sum_ref[g, :r, cols] = sum_ref[g, :r, cols] * spread(inverse, owner, q, per, r)

        by_rows(counts_ref[me, g], p, rows)
        return carry

    lax.fori_loop(0, by * bz, block, 0)


def far_kernel(dims, masks_hbm, counts_hbm, far_ref, w_ref, w_out_ref, tiled_ref, q_ref, sum_ref,
               near_m_ref, near_l_ref, out_ref, attn_ref, kv_ref, keep_ref, qs_ref, table_ref,
               masks_ref, counts_ref, m2_ref, l2_ref, acc2_ref, m_ref, l_ref, acc_ref, sems):
    by, bz, p, width, n = dims
    hd = width // HEADS
    per = TILE // hd
    copies = [
        pltpu.make_async_copy(masks_hbm, masks_ref, sems.at[0]),
        pltpu.make_async_copy(counts_hbm, counts_ref, sems.at[1]),
    ]
    for copy in copies:
        copy.start()
    me = lax.axis_index("gx")
    even = me % 2 == 0
    keep_ref[...] = jnp.zeros_like(keep_ref)

    def put(col, part):
        kv_ref[0, :, col - width : col - width + TILE] = part.astype(jnp.bfloat16)

    project(far_ref, w_ref, width, 3 * width, put)
    for copy in copies:
        copy.wait()
    other = jnp.where(even, me - 1, me + 1)
    present = (other >= 0) & (other < n)
    slabs = [(jnp.logical_not(even), jnp.clip(other, 0, n - 1), present)]

    def block(g, carry):
        j, l = g // bz, g % bz
        total, slots = compact(
            slabs, masks_ref, counts_ref, kv_ref, keep_ref, table_ref, j, l, by, bz, p
        )
        rows_out = pl.ds(pl.multiple_of(g * p, p), p)

        @pl.when(total == 0)
        def _():
            attn_ref[rows_out, :] = sum_ref[g].astype(jnp.bfloat16)

        def rows(r):
            stack_queries(q_ref, g, qs_ref, hd, r)
            attend(
                total, slots, table_ref, keep_ref, qs_ref, m_ref, l_ref, acc_ref,
                (m2_ref, l2_ref, acc2_ref), width, hd, r,
            )
            owner = lax.broadcasted_iota(jnp.int32, (r, TILE), 1) // hd
            top1, top2 = near_m_ref[g, :r, :], m_ref[:r, :]
            top = jnp.maximum(top1, top2)
            part1 = near_l_ref[g, :r, :] * jnp.exp(top1 - top)
            part2 = jnp.exp(top2 - top)
            inverse = 1.0 / (part1 + l_ref[:r, :] * part2)
            part1, part2 = part1 * inverse, part2 * inverse
            some = pl.ds(pl.multiple_of(g * p, p), r)
            for q in range(width // TILE):
                cols = slice(q * TILE, (q + 1) * TILE)
                mixed = sum_ref[g, :r, cols] * spread(part1, owner, q, per, r)
                mixed = mixed + acc_ref[:r, cols] * spread(part2, owner, q, per, r)
                attn_ref[some, cols] = mixed.astype(jnp.bfloat16)

        @pl.when(total > 0)
        def _():
            by_rows(counts_ref[me, g], p, rows)

        return carry

    lax.fori_loop(0, by * bz, block, 0)
    row = lax.broadcasted_iota(jnp.int32, (p, TILE), 0)
    for col in range(0, width, TILE):
        mixed = jnp.dot(
            attn_ref[...], w_out_ref[:, col : col + TILE], preferred_element_type=jnp.float32
        )
        for g in range(by * bz):
            part = mixed[g * p : (g + 1) * p] + tiled_ref[g, :, col : col + TILE].astype(jnp.float32)
            part = jnp.where(row < counts_ref[me, g], part, 0.0)
            out_ref[g, :, col : col + TILE] = part.astype(jnp.bfloat16)


def shards(points, order, masks, counts, gain, shift_bias, w_qkv, w_out):
    _, by, bz, p, width = points.shape
    n = lax.axis_size("gx")
    nb = by * bz
    dims = (by, bz, p, width, n)
    pairs = [e for i in range(0, n - 1, 2) for e in ((i, i + 1), (i + 1, i))]
    across = [e for i in range(1, n - 1, 2) for e in ((i, i + 1), (i + 1, i))]
    counts = counts.reshape(counts.shape[0], nb)
    pin = lambda value: pltpu.with_memory_space_constraint(value, pltpu.HBM)
    masks, counts = pin(masks), pin(counts)
    shape = jax.ShapeDtypeStruct
    dma = pltpu.SemaphoreType.DMA
    vmem = pl.BlockSpec(memory_space=pltpu.VMEM)
    hbm = pl.BlockSpec(memory_space=pltpu.HBM)
    tiled, normed = pl.pallas_call(
        functools.partial(norm_kernel, dims),
        name="norm",
        out_shape=[shape((nb, p, width), jnp.bfloat16), shape((nb * p, width), jnp.bfloat16)],
        in_specs=[hbm] * 4,
        out_specs=[vmem] * 2,
        scratch_shapes=[
            pltpu.VMEM((nb, p, width), jnp.bfloat16),
            pltpu.VMEM(order.shape, jnp.int32),
            pltpu.VMEM((1, width), jnp.float32),
            pltpu.VMEM((1, width), jnp.float32),
            dma((nb,)),
            dma((3,)),
        ],
        cost_estimate=pl.CostEstimate(
            flops=2 * nb * p * p * width, transcendentals=0, bytes_accessed=2 << 20
        ),
        compiler_params=pltpu.CompilerParams(vmem_limit_bytes=24 << 20),
    )(
        pin(points.reshape(nb, p, width)),
        pin(order),
        pin(gain.reshape(1, width)),
        pin(shift_bias.reshape(1, width)),
    )
    far = lax.ppermute(normed, "gx", across)
    pair = lax.ppermute(normed, "gx", pairs)
    slots = len(reach(by, bz))

    def scratch(slabs):
        cap = -(-slabs * slots * p // TILE) * TILE
        return [
            pltpu.VMEM((slabs, nb * p, 2 * width), jnp.bfloat16),
            pltpu.VMEM((cap, 2 * width), jnp.bfloat16),
            pltpu.VMEM((HEADS * p, TILE), jnp.bfloat16),
            pltpu.SMEM((2, slabs * slots), jnp.int32),
            pltpu.SMEM(masks.shape, jnp.int32),
            pltpu.SMEM(counts.shape, jnp.int32),
            pltpu.VMEM((p, LANES), jnp.float32),
            pltpu.VMEM((p, LANES), jnp.float32),
            pltpu.VMEM((p, width), jnp.float32),
        ]

    q, total, tops, sums = pl.pallas_call(
        functools.partial(near_kernel, dims),
        name="near",
        out_shape=[
            shape((nb, p, width), jnp.bfloat16),
            shape((nb, p, width), jnp.float32),
            shape((nb, p, LANES), jnp.float32),
            shape((nb, p, LANES), jnp.float32),
        ],
        in_specs=[hbm, hbm, vmem, vmem, hbm],
        out_specs=[vmem] * 4,
        scratch_shapes=scratch(2) + [pltpu.VMEM(w_qkv.shape, jnp.bfloat16), dma((3,))],
        cost_estimate=pl.CostEstimate(
            flops=8 * nb * p * width * 5 * width, transcendentals=0, bytes_accessed=8 << 20
        ),
        compiler_params=pltpu.CompilerParams(vmem_limit_bytes=40 << 20),
    )(masks, counts, normed, pair, pin(w_qkv))
    out = pl.pallas_call(
        functools.partial(far_kernel, dims),
        name="far",
        out_shape=shape((nb, p, width), jnp.bfloat16),
        in_specs=[hbm, hbm] + [vmem] * 8,
        out_specs=vmem,
        scratch_shapes=[pltpu.VMEM((nb * p, width), jnp.bfloat16)]
        + scratch(1)
        + [
            pltpu.VMEM((p, LANES), jnp.float32),
            pltpu.VMEM((p, LANES), jnp.float32),
            pltpu.VMEM((p, width), jnp.float32),
            dma((2,)),
        ],
        cost_estimate=pl.CostEstimate(
            flops=4 * nb * p * width * 3 * width, transcendentals=0, bytes_accessed=8 << 20
        ),
        compiler_params=pltpu.CompilerParams(vmem_limit_bytes=40 << 20),
    )(masks, counts, far, w_qkv, w_out, tiled, q, total, tops, sums)
    return out.reshape(points.shape)


def solution(mesh):
    placed = (
        P(("groups", "gx"), None, None, None, None),
        P(("groups", "gx"), None, None, None),
        P(("groups", "gx"), None, None, None),
        P("groups", None, None),
        P(),
        P(),
        P(),
        P(),
    )
    return jax.shard_map(
        shards,
        mesh=mesh,
        in_specs=placed,
        out_specs=P(("groups", "gx"), None, None, None, None),
        check_vma=False,
    )
```
